32 devices in a mesh: row: 8 (over z, core), col: 4 (over y, x).
Axes of the slice: x: 2, y: 2, z: 4, core: 2. Of those that a mesh axis runs over, the one named last changes fastest.
Arguments:
- right_sides: float32 [4, 1024, 4096], P(None, 'row', 'col'), may hold values from -6 to 6
- low_left: bfloat16 [6, 4096, 128], P(None, 'col'), may hold values from -0.25 to 0.25
- low_right: bfloat16 [6, 4096, 128], P(None, 'col'), may hold values from -0.09375 to 0.09375
- up_left: bfloat16 [6, 4096, 128], P(None, 'col'), may hold values from -0.25 to 0.25
- up_right: bfloat16 [6, 4096, 128], P(None, 'col'), may hold values from -0.09375 to 0.09375
- low_ranks: int32 [6], replicated, may hold values from 1 to 4
- up_ranks: int32 [6], replicated, may hold values from 1 to 4
- inv_lower: bfloat16 [4, 4096, 4096], P(None, 'col', 'row'), may hold values from -0.09375 to 0.09375
- inv_upper: bfloat16 [4, 4096, 4096], P(None, 'col', 'row'), may hold values from -0.09375 to 0.09375
Outputs:
- solution: float32 [4, 1024, 4096], P(None, 'row', 'col')
The draws below stay inside these ranges and needn't reach their ends.
Inputs may be any that keep to these rules, and one draw needn't show every extreme that they name: `low_ranks`: factor columns beyond 32 times this value are padding with arbitrary values and must be masked out. `up_ranks`: factor columns beyond 32 times this value are padding with arbitrary values and must be masked out.
All inputs are finite; a program needn't handle non-finite values.
Results may differ from the reference program's by a relative error of at most 0.03.
Values may be sent and summed in bfloat16 or wider, within the bound.
A program may use at most 64 MiB of HBM per device.

```python
import jax
import jax.numpy as jnp
import numpy as np
from jax import lax

B = 4096
RBLK = 32
R = 128
NT = 4
NRHS = 1024
PAIRS = 6


def touch_ends(result, rng, low, top_value):
    longest = result.shape.index(max(result.shape))
    spots = []
    for shift in (0, 1):
        where = [jax.random.randint(jax.random.fold_in(rng, axis), (), 0, length) for axis, length in enumerate(result.shape)]
        where[longest] = (where[longest] + shift) % result.shape[longest]
        spots.append(tuple(where))
    return result.at[spots[0]].set(low).at[spots[1]].set(top_value)


def shard_levels(own_key, shape, cuts, low, largest):
    loudness = 1.0
    for axis_at, blocks in cuts:
        draws = jax.random.uniform(jax.random.fold_in(jax.random.fold_in(own_key, 6), axis_at), (blocks,), jnp.float32, low / len(cuts), largest / len(cuts))
        loudness = loudness * jnp.repeat(jnp.exp(draws), shape[axis_at] // blocks).reshape((-1,) + (1,) * (len(shape) - 1 - axis_at))
    return loudness


def gaussian(stream_key, extent, deviation, bound, shards=(), held_as=jnp.bfloat16):
    values = jax.random.normal(stream_key, extent, jnp.float32) * deviation
    if len(shards) > 0:
        values = shard_levels(stream_key, extent, shards, -0.22, 0.18) * values
    return jnp.clip(values, min=-bound, max=bound).astype(held_as)


def setup_inputs(seed: int = 0) -> dict:
    arg_keys = jax.random.split(jax.random.key(seed), 10)
    return {
        "right_sides": gaussian(arg_keys[0], (NT, NRHS, B), 1.0, 6.0, ((1, 8), (2, 4)), jnp.float32),
        "low_left": gaussian(arg_keys[1], (PAIRS, B, R), (4 * R) ** -0.5, 0.25, ((1, 4),)),
        "low_right": gaussian(arg_keys[2], (PAIRS, B, R), B ** -0.5, 0.09375, ((1, 4),)),
        "up_left": gaussian(arg_keys[3], (PAIRS, B, R), (4 * R) ** -0.5, 0.25, ((1, 4),)),
        "up_right": gaussian(arg_keys[4], (PAIRS, B, R), B ** -0.5, 0.09375, ((1, 4),)),
        "low_ranks": touch_ends(jax.random.randint(arg_keys[5], (PAIRS,), 1, 5), jax.random.fold_in(arg_keys[5], 1), 1, 4).astype(jnp.int32),
        "up_ranks": touch_ends(jax.random.randint(arg_keys[6], (PAIRS,), 1, 5), jax.random.fold_in(arg_keys[6], 1), 1, 4).astype(jnp.int32),
        "inv_lower": gaussian(arg_keys[7], (NT, B, B), B ** -0.5, 0.09375, ((1, 4), (2, 8))),
        "inv_upper": gaussian(arg_keys[8], (NT, B, B), B ** -0.5, 0.09375, ((1, 4), (2, 8))),
    }


def project(solved, factors):
    return jnp.einsum("nb,mbr->mnr", solved.astype(jnp.bfloat16).astype(jnp.float32), factors.astype(jnp.float32), precision=lax.Precision.HIGHEST)


def expand(masked, factors):
    return jnp.einsum("mnr,mbr->mnb", masked.astype(jnp.float32), factors.astype(jnp.float32), precision=lax.Precision.HIGHEST)


def apply_inverse(rounded, inverse):
    return lax.dot_general(rounded, inverse, (((1,), (1,)), ((), ())), preferred_element_type=jnp.float32)


def reference(right_sides, low_left, low_right, up_left, up_right, low_ranks, up_ranks, inv_lower, inv_upper):
    columns = jnp.arange(R, dtype=jnp.int32)
    residual = right_sides
    forward = []
    for section in range(NT):
        solved = apply_inverse(residual[section].astype(jnp.bfloat16), inv_lower[section])
        forward.append(solved)
        if section + 1 < NT:
            pair_index = np.array([tile * (tile - 1) // 2 + section for tile in range(section + 1, NT)], dtype=np.int32)
            projections = project(solved, low_right[pair_index])
            rank_mask = (columns[None, :] < RBLK * low_ranks[pair_index][:, None]).astype(jnp.float32)
            masked = (projections * rank_mask[:, None, :]).astype(jnp.bfloat16)
            residual = residual.at[section + 1:].add(-expand(masked, low_left[pair_index]))
    state = jnp.stack(forward)
    solutions = [None] * NT
    for section in range(NT - 1, -1, -1):
        solved = apply_inverse(state[section].astype(jnp.bfloat16), inv_upper[section])
        solutions[section] = solved
        if section > 0:
            pair_index = np.array([section * (section - 1) // 2 + tile for tile in range(section)], dtype=np.int32)
            projections = project(solved, up_right[pair_index])
            rank_mask = (columns[None, :] < RBLK * up_ranks[pair_index][:, None]).astype(jnp.float32)
            masked = (projections * rank_mask[:, None, :]).astype(jnp.bfloat16)
            state = state.at[:section].add(-expand(masked, up_left[pair_index]))
    return jnp.stack(solutions)
```

```python
import functools

import jax
import jax.numpy as jnp
import numpy as np
from jax import lax
from jax.experimental import pallas as pl
from jax.experimental.pallas import tpu as pltpu
from jax.sharding import PartitionSpec as P

RBLK = 32


def rank_mask(ranks, pair_index, rank_cols):
    columns = jnp.arange(rank_cols, dtype=jnp.int32)
    return (columns[None, :] < RBLK * ranks[pair_index][:, None]).astype(jnp.float32)


def times_inverse(block, inverse):
    return lax.dot_general(
        block, inverse, (((1,), (1,)), ((), ())), preferred_element_type=jnp.float32
    )


def sum_terms(moved, inverse):
    return times_inverse(moved, inverse)


def shards(
    right_sides, low_left, low_right, up_left, up_right, low_ranks, up_ranks, inv_lower, inv_upper
):
    tile_count = right_sides.shape[0]
    rank_cols = low_left.shape[2]
    residual = right_sides
    forward = []
    for section in range(tile_count):
        rounded = residual[section].astype(jnp.bfloat16)
        whole = lax.all_gather(rounded, "col", axis=1, tiled=True)
        moved = lax.all_to_all(whole, "row", split_axis=1, concat_axis=0, tiled=True)
        solved = lax.psum_scatter(
            sum_terms(moved, inv_lower[section]).astype(jnp.bfloat16),
            "row",
            scatter_dimension=0,
            tiled=True,
        ).astype(jnp.float32)
        forward.append(solved)
        if section + 1 < tile_count:
            pair_index = np.array(
                [tile * (tile - 1) // 2 + section for tile in range(section + 1, tile_count)],
                dtype=np.int32,
            )
            projections = jnp.einsum(
                "nw,mwr->mnr",
                solved.astype(jnp.bfloat16),
                low_right[pair_index],
                preferred_element_type=jnp.float32,
            )
            leading = lax.psum(projections[:1].astype(jnp.bfloat16), "col").astype(jnp.float32)
            if section + 2 < tile_count:
                remaining = lax.psum(projections[1:].astype(jnp.bfloat16), "col").astype(
                    jnp.float32
                )
                summed = jnp.concatenate([leading, remaining], axis=0)
            else:
                summed = leading
            masked = (summed * rank_mask(low_ranks, pair_index, rank_cols)[:, None, :]).astype(
                jnp.bfloat16
            )
            update = jnp.einsum(
                "mnr,mwr->mnw", masked, low_left[pair_index], preferred_element_type=jnp.float32
            )
            residual = residual.at[section + 1 :].add(-update)
    state = jnp.stack(forward)
    solutions = [None] * tile_count
    for section in range(tile_count - 1, -1, -1):
        rounded = state[section].astype(jnp.bfloat16)
        whole = lax.all_gather(rounded, "col", axis=1, tiled=True)
        moved = lax.all_to_all(whole, "row", split_axis=1, concat_axis=0, tiled=True)
        solved = lax.psum_scatter(
            sum_terms(moved, inv_upper[section]).astype(jnp.bfloat16),
            "row",
            scatter_dimension=0,
            tiled=True,
        ).astype(jnp.float32)
        solutions[section] = solved
        if section > 0:
            pair_index = np.array(
                [section * (section - 1) // 2 + tile for tile in range(section)], dtype=np.int32
            )
            projections = jnp.einsum(
                "nw,mwr->mnr",
                solved.astype(jnp.bfloat16),
                up_right[pair_index],
                preferred_element_type=jnp.float32,
            )
            leading = lax.psum(projections[-1:].astype(jnp.bfloat16), "col").astype(jnp.float32)
            if section > 1:
                remaining = lax.psum(projections[:-1].astype(jnp.bfloat16), "col").astype(
                    jnp.float32
                )
                summed = jnp.concatenate([remaining, leading], axis=0)
            else:
                summed = leading
            masked = (summed * rank_mask(up_ranks, pair_index, rank_cols)[:, None, :]).astype(
                jnp.bfloat16
            )
            update = jnp.einsum(
                "mnr,mwr->mnw", masked, up_left[pair_index], preferred_element_type=jnp.float32
            )
            state = state.at[:section].add(-update)
    return jnp.stack(solutions)


MESH = pl.DeviceIdType.MESH
STREAMS = 4
LAG = {"start": 0, "spread": 1, "multiply": 2, "reduce": 3, "finish": 5}
PERIOD = 6


def schedule(streams):
    order = []
    for stream in range(streams):
        for stage, lag in LAG.items():
            at = lag + stream * PERIOD / streams
            late = int(at // PERIOD)
            order.append((at - late * PERIOD, -late, stream, stage))
    return sorted(order)


def kernel(
    shape, rhs, low_left, low_right, up_left, up_right, masks, inv_lower, inv_upper, out,
    inv, left, right, source, moved, own, other, landed, chunks, arrived, proj, proj_in,
    load_sem, g1_send, g1_recv, g2_send, g2_recv, d_send, d_recv, r_send, r_recv, p_send, p_recv,
):
    tiles, rows, cols, chips, streams, part = shape
    pairs = low_left.shape[0]
    per_col = rows // cols
    lanes = inv_lower.shape[2]
    piece = lanes // cols
    row, col = lax.axis_index("row"), lax.axis_index("col")
    chip, core = lax.div(row, 2), lax.rem(row, 2)
    home = lax.div(row, per_col)

    loads = [(rhs, out)]
    loads += [(inv_lower.at[k], inv.at[k]) for k in range(tiles)]
    loads += [(low_right, right.at[pl.ds(0, pairs)]), (low_left, left.at[pl.ds(0, pairs)])]
    loads += [(up_right, right.at[pl.ds(pairs, pairs)]), (up_left, left.at[pl.ds(pairs, pairs)])]
    loads += [(inv_upper.at[k], inv.at[2 * tiles - 1 - k]) for k in range(tiles - 1, -1, -1)]
    slots = [0] + list(range(1, 1 + tiles)) + [2 * tiles + 1 + k for k in range(4)]
    slots += list(range(1 + tiles, 1 + 2 * tiles))
    copies = [pltpu.make_async_copy(a, b, load_sem.at[s]) for (a, b), s in zip(loads, slots)]
    for copy in copies:
        copy.start()
    proj[...] = jnp.zeros_like(proj)
    copies[0].wait()

    def remote(src, dst, send, recv, to_row, to_col):
        return pltpu.make_async_remote_copy(
            src_ref=src, dst_ref=dst, send_sem=send, recv_sem=recv,
            device_id=(to_row, to_col), device_id_type=MESH,
        )

    def own_lanes():
        return pl.ds(pl.multiple_of(col * piece, piece), piece)

    def geometry(step):
        back = lax.div(step, tiles)
        section = step + back * (2 * tiles - 1 - 2 * step)
        count = (1 - back) * (tiles - 1 - section) + back * section
        return back, section, count

    def tile_of(back, section, u):
        tile = (1 - back) * (section + 1) + u
        pair = (1 - back) * (lax.div(tile * (tile + 2 * tiles - 1), 2) - tile * tiles + section)
        pair = pair + back * (pairs + lax.div(section * (section + 2 * tiles - 1), 2) - section * tiles + u)
        return tile, pair

    def place(stream):
        return pl.ds(stream * part, part)

    def g1(step, stream, half, q):
        side = lax.rem(step, 2)
        return remote(
            source.at[stream, :, pl.ds(half * lanes + q * piece, piece)],
            moved.at[side, stream, core, chip, :, pl.ds(q * piece, piece)],
            g1_send.at[stream, half * cols + q],
            g1_recv.at[stream, side, row],
            col * per_col + half,
            q,
        )

    def g1_mine(half, q):
        return jnp.logical_and(row == col * per_col + half, col == q)

    def g2(step, stream, hop):
        side = lax.rem(step, 2)
        view = moved.at[side, stream, :, :, :, own_lanes()]
        return remote(
            view, view, g2_send.at[stream, hop], g2_recv.at[stream, side, hop],
            row, lax.rem(col + hop, cols),
        )

    def swap(step, stream):
        side = lax.rem(step, 2)
        return remote(
            other.at[stream], landed.at[side, stream], d_send.at[stream], d_recv.at[stream, side],
            row + 1 - 2 * core, col,
        )

    def scatter(step, stream, hop):
        side = lax.rem(step, 2)
        to = lax.rem(chip + hop, chips)
        return remote(
            chunks.at[stream, to], arrived.at[side, stream, hop],
            r_send.at[stream, hop], r_recv.at[stream, side, hop],
            2 * to + core, col,
        )

    def project(step, stream, hop):
        side = lax.rem(step, 2)
        return remote(
            proj.at[stream], proj_in.at[side, stream, hop],
            p_send.at[stream, hop], p_recv.at[stream, side, hop],
            row, lax.rem(col + hop, cols),
        )

    def update(step, stream):
        back, section, count = geometry(step)
        side = lax.rem(step, 2)
        for hop in range(1, cols):
            project(step, stream, hop).wait()

        def one(u, carry):
            tile, pair = tile_of(back, section, u)
            total = proj[stream, u].astype(jnp.float32)
            for hop in range(1, cols):
                total += proj_in[side, stream, hop, u].astype(jnp.float32)
            masked = (total * masks[pair]).astype(jnp.bfloat16)
            out[tile, place(stream), :] -= times_inverse(masked, left[pair])
            return carry

        lax.fori_loop(0, count, one, 0)

    def start(step, stream):
        @pl.when(jnp.logical_and(step > 0, step != tiles))
        def _():
            update(step - 1, stream)

        _, section, _ = geometry(step)
        source[stream] = out[section, place(stream), :].astype(jnp.bfloat16)
        for half in range(per_col):
            for q in range(cols):
                copy = g1(step, stream, half, q)
                mine = g1_mine(half, q)

                @pl.when(jnp.logical_not(mine))
                def _():
                    copy.start()

                @pl.when(mine)
                def _():
                    pltpu.make_async_copy(
                        copy.src_ref, copy.dst_ref, g1_recv.at[stream, lax.rem(step, 2), row]
                    ).start()

    def spread(step, stream):
        side = lax.rem(step, 2)
        for k in range(rows):
            view = moved.at[side, stream, k % 2, k // 2, :, own_lanes()]
            pltpu.make_async_copy(view, view, g1_recv.at[stream, side, k]).wait()
        for hop in range(1, cols):
            g2(step, stream, hop).start()
        for half in range(per_col):
            for q in range(cols):

                @pl.when(jnp.logical_not(g1_mine(half, q)))
                def _():
                    g1(step, stream, half, q).wait_send()

    def multiply(step, stream):
        side = lax.rem(step, 2)
        if stream == 0:
            pltpu.make_async_copy(inv_lower.at[0], inv.at[step], load_sem.at[1 + step]).wait()
        for hop in range(1, cols):
            view = moved.at[
                side, stream, :, :, :,
                pl.ds(pl.multiple_of(lax.rem(col + cols - hop, cols) * piece, piece), piece),
            ]
            pltpu.make_async_copy(view, view, g2_recv.at[stream, side, hop]).wait()
        theirs = moved[side, stream, 1 - core].reshape(chips * part, lanes)
        other[stream] = (
            times_inverse(theirs, inv[step]).astype(jnp.bfloat16).reshape(chips, part, -1)
        )
        swap(step, stream).start()
        ours = moved[side, stream, core].reshape(chips * part, lanes)
        own[stream] = times_inverse(ours, inv[step]).reshape(chips, part, -1)
        for hop in range(1, cols):
            g2(step, stream, hop).wait_send()

    def reduce(step, stream):
        side = lax.rem(step, 2)
        swap(step, stream).wait()
        for hop in list(range(1, chips)):
            to = lax.rem(chip + hop, chips)
            chunks[stream, to] = (
                own[stream, to] + landed[side, stream, to].astype(jnp.float32)
            ).astype(jnp.bfloat16)
            scatter(step, stream, hop).start()

    def finish(step, stream):
        side = lax.rem(step, 2)
        back, section, count = geometry(step)
        total = own[stream, chip] + landed[side, stream, chip].astype(jnp.float32)
        for hop in range(1, chips):
            scatter(step, stream, hop).wait()
            total += arrived[side, stream, hop].astype(jnp.float32)
        out[section, place(stream), :] = total
        if stream == 0:

            @pl.when(step == 0)
            def _():
                for k in range(1 + tiles, 5 + tiles):
                    copies[k].wait()

        @pl.when(count > 0)
        def _():
            rounded = out[section, place(stream), :].astype(jnp.bfloat16)

            def one(u, carry):
                _, pair = tile_of(back, section, u)
                proj[stream, u] = jnp.dot(
                    rounded, right[pair], preferred_element_type=jnp.float32
                ).astype(jnp.bfloat16)
                return carry

            lax.fori_loop(0, count, one, 0)
            for hop in range(1, cols):
                project(step, stream, hop).start()

    stages = {
        "start": start, "spread": spread, "multiply": multiply, "reduce": reduce, "finish": finish,
    }
    steps = 2 * tiles
    order = schedule(streams)
    latest = -min(shift for _, shift, _, _ in order)

    def body(turn, carry):
        for _, shift, stream, stage in order:
            step = turn + shift

            @pl.when(jnp.logical_and(step >= 0, step < steps))
            def _():
                stages[stage](step, stream)

        return carry

    lax.fori_loop(0, steps + latest, body, 0)


def fused(
    rows, cols, streams, right_sides, low_left, low_right, up_left, up_right, low_ranks, up_ranks,
    inv_lower, inv_upper,
):
    tiles, held, wide = right_sides.shape
    pairs, _, rank_cols = low_left.shape
    lanes = inv_lower.shape[2]
    chips = rows // 2
    part = held // streams
    masks = rank_mask(
        jnp.concatenate([low_ranks, up_ranks]), np.arange(2 * pairs), rank_cols
    ).reshape(2 * pairs, 1, rank_cols)
    half = jnp.bfloat16
    dma = pltpu.SemaphoreType.DMA
    scratch = [
        pltpu.VMEM((2 * tiles, wide, lanes), half),
        pltpu.VMEM((2 * pairs, wide, rank_cols), half),
        pltpu.VMEM((2 * pairs, wide, rank_cols), half),
        pltpu.VMEM((streams, part, wide), half),
        pltpu.VMEM((2, streams, 2, chips, part, lanes), half),
        pltpu.VMEM((streams, chips, part, wide), jnp.float32),
        pltpu.VMEM((streams, chips, part, wide), half),
        pltpu.VMEM((2, streams, chips, part, wide), half),
        pltpu.VMEM((streams, chips, part, wide), half),
        pltpu.VMEM((2, streams, chips, part, wide), half),
        pltpu.VMEM((streams, tiles - 1, part, rank_cols), half),
        pltpu.VMEM((2, streams, cols, tiles - 1, part, rank_cols), half),
        dma((2 * tiles + 5,)),
        dma((streams, rows)), dma((streams, 2, rows)),
        dma((streams, cols)), dma((streams, 2, cols)),
        dma((streams,)), dma((streams, 2)),
        dma((streams, chips)), dma((streams, 2, chips)),
        dma((streams, cols)), dma((streams, 2, cols)),
    ]
    anywhere = pl.BlockSpec(memory_space=pl.ANY)
    vmem = pl.BlockSpec(memory_space=pltpu.VMEM)
    return pl.pallas_call(
        functools.partial(kernel, (tiles, rows, cols, chips, streams, part)),
        out_shape=jax.ShapeDtypeStruct(right_sides.shape, jnp.float32),
        in_specs=[anywhere] * 5 + [vmem] + [anywhere] * 2,
        out_specs=vmem,
        scratch_shapes=scratch,
        compiler_params=pltpu.CompilerParams(
            has_side_effects=True, vmem_limit_bytes=60 * 1024 * 1024
        ),
    )(right_sides, low_left, low_right, up_left, up_right, masks, inv_lower, inv_upper)


def pick(mesh):
    rows, cols = mesh.shape["row"], mesh.shape["col"]

    def run(right_sides, *rest):
        held, lanes = right_sides.shape[1], rest[-1].shape[2]
        fits = rows % 2 == 0 and rows % cols == 0 and lanes % (128 * cols) == 0
        if fits and held % (16 * STREAMS) == 0:
            return fused(rows, cols, STREAMS, right_sides, *rest)
        return shards(right_sides, *rest)

    return run


def solution(mesh):
    in_specs = (
        P(None, "row", "col"),
        P(None, "col", None),
        P(None, "col", None),
        P(None, "col", None),
        P(None, "col", None),
        P(),
        P(),
        P(None, "col", "row"),
        P(None, "col", "row"),
    )
    out_specs = P(None, "row", "col")
    return jax.shard_map(pick(mesh), mesh=mesh, in_specs=in_specs, out_specs=out_specs, check_vma=False)
```

```python
import functools

import jax
import jax.numpy as jnp
import numpy as np
from jax import lax
from jax.experimental import pallas as pl
from jax.experimental.pallas import tpu as pltpu
from jax.sharding import PartitionSpec as P

RBLK = 32


def rank_mask(ranks, pair_index, rank_cols):
    columns = jnp.arange(rank_cols, dtype=jnp.int32)
    return (columns[None, :] < RBLK * ranks[pair_index][:, None]).astype(jnp.float32)


def times_inverse(block, inverse):
    return lax.dot_general(
        block, inverse, (((1,), (1,)), ((), ())), preferred_element_type=jnp.float32
    )


def sum_terms(moved, inverse):
    return times_inverse(moved, inverse)


def shards(
    right_sides, low_left, low_right, up_left, up_right, low_ranks, up_ranks, inv_lower, inv_upper
):
    tile_count = right_sides.shape[0]
    rank_cols = low_left.shape[2]
    residual = right_sides
    forward = []
    for section in range(tile_count):
        rounded = residual[section].astype(jnp.bfloat16)
        whole = lax.all_gather(rounded, "col", axis=1, tiled=True)
        moved = lax.all_to_all(whole, "row", split_axis=1, concat_axis=0, tiled=True)
        solved = lax.psum_scatter(
            sum_terms(moved, inv_lower[section]).astype(jnp.bfloat16),
            "row",
            scatter_dimension=0,
            tiled=True,
        ).astype(jnp.float32)
        forward.append(solved)
        if section + 1 < tile_count:
            pair_index = np.array(
                [tile * (tile - 1) // 2 + section for tile in range(section + 1, tile_count)],
                dtype=np.int32,
            )
            projections = jnp.einsum(
                "nw,mwr->mnr",
                solved.astype(jnp.bfloat16),
                low_right[pair_index],
                preferred_element_type=jnp.float32,
            )
            leading = lax.psum(projections[:1].astype(jnp.bfloat16), "col").astype(jnp.float32)
            if section + 2 < tile_count:
                remaining = lax.psum(projections[1:].astype(jnp.bfloat16), "col").astype(
                    jnp.float32
                )
                summed = jnp.concatenate([leading, remaining], axis=0)
            else:
                summed = leading
            masked = (summed * rank_mask(low_ranks, pair_index, rank_cols)[:, None, :]).astype(
                jnp.bfloat16
            )
            update = jnp.einsum(
                "mnr,mwr->mnw", masked, low_left[pair_index], preferred_element_type=jnp.float32
            )
            residual = residual.at[section + 1 :].add(-update)
    state = jnp.stack(forward)
    solutions = [None] * tile_count
    for section in range(tile_count - 1, -1, -1):
        rounded = state[section].astype(jnp.bfloat16)
        whole = lax.all_gather(rounded, "col", axis=1, tiled=True)
        moved = lax.all_to_all(whole, "row", split_axis=1, concat_axis=0, tiled=True)
        solved = lax.psum_scatter(
            sum_terms(moved, inv_upper[section]).astype(jnp.bfloat16),
            "row",
            scatter_dimension=0,
            tiled=True,
        ).astype(jnp.float32)
        solutions[section] = solved
        if section > 0:
            pair_index = np.array(
                [section * (section - 1) // 2 + tile for tile in range(section)], dtype=np.int32
            )
            projections = jnp.einsum(
                "nw,mwr->mnr",
                solved.astype(jnp.bfloat16),
                up_right[pair_index],
                preferred_element_type=jnp.float32,
            )
            leading = lax.psum(projections[-1:].astype(jnp.bfloat16), "col").astype(jnp.float32)
            if section > 1:
                remaining = lax.psum(projections[:-1].astype(jnp.bfloat16), "col").astype(
                    jnp.float32
                )
                summed = jnp.concatenate([remaining, leading], axis=0)
            else:
                summed = leading
            masked = (summed * rank_mask(up_ranks, pair_index, rank_cols)[:, None, :]).astype(
                jnp.bfloat16
            )
            update = jnp.einsum(
                "mnr,mwr->mnw", masked, up_left[pair_index], preferred_element_type=jnp.float32
            )
            state = state.at[:section].add(-update)
    return jnp.stack(solutions)


MESH = pl.DeviceIdType.MESH
STREAMS = 4
LAG = {"start": 0, "spread": 0.7, "multiply": 1.4, "reduce": 1.65, "relay": 2.6, "finish": 3.5}
PERIOD = 4


def schedule(streams):
    order = []
    for stream in range(streams):
        for stage, lag in LAG.items():
            at = lag + stream * PERIOD / streams
            late = int(at // PERIOD)
            order.append((at - late * PERIOD, -late, stream, stage))
    return sorted(order)


def kernel(
    shape, rhs, low_left, low_right, up_left, up_right, masks, inv_lower, inv_upper, out,
    inv, left, right, source, moved, own, other, landed, chunks, arrived, proj, proj_in,
    load_sem, g1_send, g1_recv, g2_send, g2_recv, d_send, d_recv, r_send, r_recv, p_send, p_recv,
):
    tiles, rows, cols, chips, streams, part = shape
    pairs = low_left.shape[0]
    per_col = rows // cols
    lanes = inv_lower.shape[2]
    piece = lanes // cols
    row, col = lax.axis_index("row"), lax.axis_index("col")
    chip, core = lax.div(row, 2), lax.rem(row, 2)
    pair_at, member, pair_count = lax.div(chip, 2), lax.rem(chip, 2), chips // 2

    loads = [(rhs, out)]
    loads += [(inv_lower.at[k], inv.at[k]) for k in range(tiles)]
    loads += [(low_right, right.at[pl.ds(0, pairs)]), (low_left, left.at[pl.ds(0, pairs)])]
    loads += [(up_right, right.at[pl.ds(pairs, pairs)]), (up_left, left.at[pl.ds(pairs, pairs)])]
    loads += [(inv_upper.at[k], inv.at[2 * tiles - 1 - k]) for k in range(tiles - 1, -1, -1)]
    slots = [0] + list(range(1, 1 + tiles)) + [2 * tiles + 1 + k for k in range(4)]
    slots += list(range(1 + tiles, 1 + 2 * tiles))
    copies = [pltpu.make_async_copy(a, b, load_sem.at[s]) for (a, b), s in zip(loads, slots)]
    for copy in copies:
        copy.start()
    proj[...] = jnp.zeros_like(proj)
    copies[0].wait()

    def remote(src, dst, send, recv, to_row, to_col):
        return pltpu.make_async_remote_copy(
            src_ref=src, dst_ref=dst, send_sem=send, recv_sem=recv,
            device_id=(to_row, to_col), device_id_type=MESH,
        )

    def own_lanes():
        return pl.ds(pl.multiple_of(col * piece, piece), piece)

    def geometry(step):
        back = lax.div(step, tiles)
        section = step + back * (2 * tiles - 1 - 2 * step)
        count = (1 - back) * (tiles - 1 - section) + back * section
        return back, section, count

    def tile_of(back, section, u):
        tile = (1 - back) * (section + 1) + u
        pair = (1 - back) * (lax.div(tile * (tile + 2 * tiles - 1), 2) - tile * tiles + section)
        pair = pair + back * (pairs + lax.div(section * (section + 2 * tiles - 1), 2) - section * tiles + u)
        return tile, pair

    def place(stream):
        return pl.ds(stream * part, part)

    def g1(step, stream, half, q):
        side = lax.rem(step, 2)
        return remote(
            source.at[stream, :, pl.ds(half * lanes + q * piece, piece)],
            moved.at[side, stream, core, chip, :, pl.ds(q * piece, piece)],
            g1_send.at[stream, half * cols + q],
            g1_recv.at[stream, side, row],
            col * per_col + half,
            q,
        )

    def g1_mine(half, q):
        return jnp.logical_and(row == col * per_col + half, col == q)

    def g2(step, stream, hop):
        side = lax.rem(step, 2)
        view = moved.at[side, stream, :, :, :, own_lanes()]
        return remote(
            view, view, g2_send.at[stream, hop], g2_recv.at[stream, side, hop],
            row, lax.rem(col + hop, cols),
        )

    def swap(step, stream):
        side = lax.rem(step, 2)
        return remote(
            other.at[stream], landed.at[side, stream], d_send.at[stream], d_recv.at[stream, side],
            row + 1 - 2 * core, col,
        )

    def pass_on(step, stream, slot, to):
        side = lax.rem(step, 2)
        return remote(
            chunks.at[stream, slot], arrived.at[side, stream, slot],
            r_send.at[stream, slot], r_recv.at[stream, side, slot],
            2 * to + core, col,
        )

    def pair_copy(step, stream, hop):
        return pass_on(step, stream, hop, chip + 1 - 2 * member)

    def relay_copy(step, stream, hop):
        return pass_on(step, stream, pair_count + hop, 2 * lax.rem(pair_at + hop, pair_count) + member)

    def held_sum(step, stream, to):
        return own[stream, to] + landed[lax.rem(step, 2), stream, to].astype(jnp.float32)

    def project(step, stream, hop):
        side = lax.rem(step, 2)
        return remote(
            proj.at[stream], proj_in.at[side, stream, hop],
            p_send.at[stream, hop], p_recv.at[stream, side, hop],
            row, lax.rem(col + hop, cols),
        )

    def update(step, stream):
        back, section, count = geometry(step)
        side = lax.rem(step, 2)
        for hop in range(1, cols):
            project(step, stream, hop).wait()

        def one(u, carry):
            tile, pair = tile_of(back, section, u)
            total = proj[stream, u].astype(jnp.float32)
            for hop in range(1, cols):
                total += proj_in[side, stream, hop, u].astype(jnp.float32)
            masked = (total * masks[pair]).astype(jnp.bfloat16)
            out[tile, place(stream), :] -= times_inverse(masked, left[pair])
            return carry

        lax.fori_loop(0, count, one, 0)

    def start(step, stream):
        @pl.when(jnp.logical_and(step > 0, step != tiles))
        def _():
            update(step - 1, stream)

        _, section, _ = geometry(step)
        source[stream] = out[section, place(stream), :].astype(jnp.bfloat16)
        for half in range(per_col):
            for q in range(cols):
                copy = g1(step, stream, half, q)
                mine = g1_mine(half, q)

                @pl.when(jnp.logical_not(mine))
                def _():
                    copy.start()

                @pl.when(mine)
                def _():
                    pltpu.make_async_copy(
                        copy.src_ref, copy.dst_ref, g1_recv.at[stream, lax.rem(step, 2), row]
                    ).start()

    def spread(step, stream):
        side = lax.rem(step, 2)
        for k in range(rows):
            view = moved.at[side, stream, k % 2, k // 2, :, own_lanes()]
            pltpu.make_async_copy(view, view, g1_recv.at[stream, side, k]).wait()
        for hop in range(1, cols):
            g2(step, stream, hop).start()
        for half in range(per_col):
            for q in range(cols):

                @pl.when(jnp.logical_not(g1_mine(half, q)))
                def _():
                    g1(step, stream, half, q).wait_send()

    def multiply(step, stream):
        side = lax.rem(step, 2)
        if stream == 0:
            pltpu.make_async_copy(inv_lower.at[0], inv.at[step], load_sem.at[1 + step]).wait()
        for hop in range(1, cols):
            view = moved.at[
                side, stream, :, :, :,
                pl.ds(pl.multiple_of(lax.rem(col + cols - hop, cols) * piece, piece), piece),
            ]
            pltpu.make_async_copy(view, view, g2_recv.at[stream, side, hop]).wait()
        theirs = moved[side, stream, 1 - core].reshape(chips * part, lanes)
        other[stream] = (
            times_inverse(theirs, inv[step]).astype(jnp.bfloat16).reshape(chips, part, -1)
        )
        swap(step, stream).start()
        ours = moved[side, stream, core].reshape(chips * part, lanes)
        own[stream] = times_inverse(ours, inv[step]).reshape(chips, part, -1)
        for hop in range(1, cols):
            g2(step, stream, hop).wait_send()

    def reduce(step, stream):
        swap(step, stream).wait()
        for hop in list(range(1, pair_count)) + [0]:
            to = 2 * lax.rem(pair_at + hop, pair_count) + 1 - member
            chunks[stream, hop] = held_sum(step, stream, to).astype(jnp.bfloat16)
            pair_copy(step, stream, hop).start()

    def relay(step, stream):
        side = lax.rem(step, 2)
        for hop in range(1, pair_count):
            pair_copy(step, stream, hop).wait()
            to = 2 * lax.rem(pair_at + hop, pair_count) + member
            total = held_sum(step, stream, to) + arrived[side, stream, hop].astype(jnp.float32)
            chunks[stream, pair_count + hop] = total.astype(jnp.bfloat16)
            relay_copy(step, stream, hop).start()

    def finish(step, stream):
        side = lax.rem(step, 2)
        back, section, count = geometry(step)
        total = held_sum(step, stream, chip)
        pair_copy(step, stream, 0).wait()
        total += arrived[side, stream, 0].astype(jnp.float32)
        for hop in range(1, pair_count):
            relay_copy(step, stream, hop).wait()
            total += arrived[side, stream, pair_count + hop].astype(jnp.float32)
        out[section, place(stream), :] = total
        if stream == 0:

            @pl.when(step == 0)
            def _():
                for k in range(1 + tiles, 5 + tiles):
                    copies[k].wait()

        @pl.when(count > 0)
        def _():
            rounded = out[section, place(stream), :].astype(jnp.bfloat16)

            def one(u, carry):
                _, pair = tile_of(back, section, u)
                proj[stream, u] = jnp.dot(
                    rounded, right[pair], preferred_element_type=jnp.float32
                ).astype(jnp.bfloat16)
                return carry

            lax.fori_loop(0, count, one, 0)
            for hop in range(1, cols):
                project(step, stream, hop).start()

    stages = {
        "start": start, "spread": spread, "multiply": multiply, "reduce": reduce, "relay": relay,
        "finish": finish,
    }
    steps = 2 * tiles
    order = schedule(streams)
    latest = -min(shift for _, shift, _, _ in order)

    def body(turn, carry):
        for _, shift, stream, stage in order:
            step = turn + shift

            @pl.when(jnp.logical_and(step >= 0, step < steps))
            def _():
                stages[stage](step, stream)

        return carry

    lax.fori_loop(0, steps + latest, body, 0)


def fused(
    rows, cols, streams, right_sides, low_left, low_right, up_left, up_right, low_ranks, up_ranks,
    inv_lower, inv_upper,
):
    tiles, held, wide = right_sides.shape
    pairs, _, rank_cols = low_left.shape
    lanes = inv_lower.shape[2]
    chips = rows // 2
    part = held // streams
    masks = rank_mask(
        jnp.concatenate([low_ranks, up_ranks]), np.arange(2 * pairs), rank_cols
    ).reshape(2 * pairs, 1, rank_cols)
    half = jnp.bfloat16
    dma = pltpu.SemaphoreType.DMA
    scratch = [
        pltpu.VMEM((2 * tiles, wide, lanes), half),
        pltpu.VMEM((2 * pairs, wide, rank_cols), half),
        pltpu.VMEM((2 * pairs, wide, rank_cols), half),
        pltpu.VMEM((streams, part, wide), half),
        pltpu.VMEM((2, streams, 2, chips, part, lanes), half),
        pltpu.VMEM((streams, chips, part, wide), jnp.float32),
        pltpu.VMEM((streams, chips, part, wide), half),
        pltpu.VMEM((2, streams, chips, part, wide), half),
        pltpu.VMEM((streams, chips, part, wide), half),
        pltpu.VMEM((2, streams, chips, part, wide), half),
        pltpu.VMEM((streams, tiles - 1, part, rank_cols), half),
        pltpu.VMEM((2, streams, cols, tiles - 1, part, rank_cols), half),
        dma((2 * tiles + 5,)),
        dma((streams, rows)), dma((streams, 2, rows)),
        dma((streams, cols)), dma((streams, 2, cols)),
        dma((streams,)), dma((streams, 2)),
        dma((streams, chips)), dma((streams, 2, chips)),
        dma((streams, cols)), dma((streams, 2, cols)),
    ]
    anywhere = pl.BlockSpec(memory_space=pl.ANY)
    vmem = pl.BlockSpec(memory_space=pltpu.VMEM)
    return pl.pallas_call(
        functools.partial(kernel, (tiles, rows, cols, chips, streams, part)),
        out_shape=jax.ShapeDtypeStruct(right_sides.shape, jnp.float32),
        in_specs=[anywhere] * 5 + [vmem] + [anywhere] * 2,
        out_specs=vmem,
        scratch_shapes=scratch,
        compiler_params=pltpu.CompilerParams(
            has_side_effects=True, vmem_limit_bytes=60 * 1024 * 1024
        ),
    )(right_sides, low_left, low_right, up_left, up_right, masks, inv_lower, inv_upper)


def pick(mesh):
    rows, cols = mesh.shape["row"], mesh.shape["col"]

    def run(right_sides, *rest):
        held, lanes = right_sides.shape[1], rest[-1].shape[2]
        fits = rows % 4 == 0 and rows % cols == 0 and lanes % (128 * cols) == 0
        if fits and held % (16 * STREAMS) == 0:
            return fused(rows, cols, STREAMS, right_sides, *rest)
        return shards(right_sides, *rest)

    return run


def solution(mesh):
    in_specs = (
        P(None, "row", "col"),
        P(None, "col", None),
        P(None, "col", None),
        P(None, "col", None),
        P(None, "col", None),
        P(),
        P(),
        P(None, "col", "row"),
        P(None, "col", "row"),
    )
    out_specs = P(None, "row", "col")
    return jax.shard_map(pick(mesh), mesh=mesh, in_specs=in_specs, out_specs=out_specs, check_vma=False)
```
